32 devices in a mesh: out: 8 (over z, x), inp: 4 (over y, core).
Axes of the slice: x: 2, y: 2, z: 4, core: 2. Of those that a mesh axis runs over, the one named last changes fastest.
Arguments:
- tensor: bfloat16 [1024, 1024, 1024], P('out', 'inp'), may hold values from -0.005859375 to 0.005859375
- state: bfloat16 [768, 1024], P('out'), may hold values from -6 to 6
Outputs:
- collision: bfloat16 [768, 1024], P('inp', 'out')
The draws below stay inside these ranges and needn't reach their ends.
All inputs are finite; a program needn't handle non-finite values.
Results may differ from the reference program's by a relative error of at most 0.001.
Values may be sent and summed in bfloat16 or wider, within the bound.
A program may use at most 128 MiB of HBM per device.

```python
import jax
import jax.numpy as jnp
from jax import lax

K = 1024
CELLS = 768


def shard_levels(key, shape, split, least, high):
    loudness, own = 1.0, jax.random.fold_in(key, 6)
    for dim, shards_of in split:
        steps = jnp.exp(jax.random.uniform(jax.random.fold_in(own, dim), (shards_of,), jnp.float32, least / len(split), high / len(split)))
        loudness = loudness * jnp.repeat(steps, shape[dim] // shards_of).reshape([-1 if axis == dim else 1 for axis in range(len(shape))])
    return loudness


def centred(own_key, extent, scale, most, shards=(), kind=jnp.bfloat16):
    drawn = jax.random.normal(own_key, extent, jnp.float32) * scale
    if len(shards) > 0:
        drawn = shard_levels(own_key, extent, shards, -0.22, 0.18) * drawn
    return jnp.clip(drawn, min=-most, max=most).astype(kind)


def setup_inputs(seed: int = 0) -> dict:
    key_list = jax.random.split(jax.random.key(seed), 3)
    return {
        "tensor": centred(key_list[0], (K, K, K), (K * K) ** -0.5, 0.005859375, ((0, 8), (1, 4))),
        "state": centred(key_list[1], (CELLS, K), 1.0, 6.0, ((0, 8),)),
    }


def reference(tensor, state):
    blocks = tensor.reshape(K // 16, 16, K, K)
    state_wide = state.astype(jnp.float32)

    def one_block(slab):
        flat = slab.reshape(16 * K, K)
        inner = lax.dot_general(state, flat, (((1,), (1,)), ((), ())), preferred_element_type=jnp.float32)
        inner = inner.reshape(state.shape[0], 16, K)
        return jnp.sum(inner * state_wide[:, None, :], axis=2)

    parts = lax.map(one_block, blocks)
    result = jnp.transpose(parts, (1, 0, 2)).reshape(state.shape[0], K)
    return result.astype(jnp.bfloat16)
```

```python
import functools

import jax
import jax.numpy as jnp
from jax import lax
from jax.experimental import pallas as pl
from jax.experimental.pallas import tpu as pltpu
from jax.sharding import PartitionSpec as P

MESH = pl.DeviceIdType.MESH
GROUP = 8
SLOTS = 4


def kernel(nx, n_out, n_inp, tensor, state, out, gathered, turned, chosen, slab, parts, landed,
           own_sems, z_sems, x_sems, core_sems, t_sems, s_sems, r_sems):
    rows_out, rows_inp, width = tensor.shape
    cells_own = state.shape[0]
    cells = n_out * cells_own
    nz = n_out // nx
    per_owner = n_out // n_inp
    blocks = rows_out // GROUP
    slots = slab.shape[0]
    lanes = 256 if cells % 256 == 0 else cells
    halves = 2
    half_width = width // halves

    me_o = lax.axis_index("out")
    me_p = lax.axis_index("inp")
    z, x = me_o // nx, me_o % nx
    half = me_p % halves
    partner = me_p + 1 - 2 * half
    cols = pl.ds(pl.multiple_of(half * half_width, 128), half_width)
    other_cols = pl.ds(pl.multiple_of((1 - half) * half_width, 128), half_width)

    def fetch(b, slot):
        return pltpu.make_async_copy(
            tensor.at[pl.ds(b * GROUP, GROUP)], slab.at[slot], t_sems.at[slot])

    for b in range(min(slots, blocks)):
        fetch(b, b).start()

    def out_of(zz, xx):
        return lax.rem(zz + nz, nz) * nx + lax.rem(xx + nx, nx)

    barrier = pltpu.get_barrier_semaphore()
    near = [(out_of(z + d, x), me_p) for d in range(1, nz)]
    near += [(out_of(z, x + e), me_p) for e in range(1, nx)]
    near += [(me_o, lax.rem(me_p + q, n_inp)) for q in range(1, n_inp)]
    for device in near:
        pl.semaphore_signal(barrier, inc=1, device_id=device, device_id_type=MESH)
    pl.semaphore_wait(barrier, len(near))

    def remote(src, dst, send, recv, device):
        return pltpu.make_async_remote_copy(
            src_ref=src, dst_ref=dst, send_sem=send, recv_sem=recv,
            device_id=device, device_id_type=MESH)

    def z_copy(d):
        return remote(state.at[:, cols], gathered.at[me_o, :, cols], z_sems.at[0, d],
                      z_sems.at[1, d], (out_of(z + d, x), me_p))

    def x_copy(e, d):
        shard = out_of(z - d, x)
        src = state.at[:, cols] if d == 0 else gathered.at[shard, :, cols]
        return remote(src, gathered.at[shard, :, cols], x_sems.at[0, e, d], x_sems.at[1, e, d],
                      (out_of(z, x + e), me_p))

    def core_copy(e, d):
        shard = out_of(z - d, x - e)
        block = gathered.at[shard, :, cols]
        return remote(block, block, core_sems.at[0, e, d], core_sems.at[1, e, d], (me_o, partner))

    started = []

    def start(copy):
        copy.start()
        started.append(copy)

    for e in range(1, nx):
        start(x_copy(e, 0))
    for d in range(1, nz):
        start(z_copy(d))
    gathered[me_o] = state[...]
    for e in range(1, nx):
        x_copy(e, 0).wait_recv()
        start(core_copy(e, 0))
    for d in range(1, nz):
        z_copy(d).wait_recv()
        for e in range(1, nx):
            start(x_copy(e, d))
        start(core_copy(0, d))
    for d in range(1, nz):
        for e in range(1, nx):
            x_copy(e, d).wait_recv()
            start(core_copy(e, d))
    for d in range(nz):
        for e in range(nx):
            if (e, d) != (0, 0):
                core_copy(e, d).wait_recv()

    for j in range(0, width, 128):
        piece = gathered[:, :, j:j + 128].reshape(cells, 128)
        turned[j:j + 128, :] = piece.T
    first = pl.multiple_of(me_p * rows_inp, rows_inp)
    chosen[...] = turned[pl.ds(first, rows_inp), :].astype(jnp.float32)

    def send_part(b, q):
        owner = lax.rem(me_p + q, n_inp)
        rows = pl.ds(pl.multiple_of(b * GROUP, GROUP), GROUP)
        return remote(parts.at[pl.ds(owner * per_owner, per_owner), rows],
                      landed.at[q - 1, :, rows],
                      s_sems.at[q - 1], r_sems.at[q - 1], (me_o, owner))

    def compute(b, carry):
        slot = lax.rem(b, slots)
        fetch(b, slot).wait()
        pieces = []
        for n in range(0, cells, lanes):
            sums = []
            for k in range(GROUP):
                inner = jnp.dot(slab[slot, k], turned[:, n:n + lanes],
                                preferred_element_type=jnp.float32)
                sums.append(jnp.sum(inner * chosen[:, n:n + lanes], axis=0, keepdims=True))
            pieces.append(jnp.concatenate(sums, axis=0))
        total = jnp.concatenate(pieces, axis=1)
        rows = pl.ds(pl.multiple_of(b * GROUP, GROUP), GROUP)
        for s in range(n_out):
            parts[s, rows, 0:cells_own] = total[:, s * cells_own:(s + 1) * cells_own]

        @pl.when(b + slots < blocks)
        def _():
            fetch(b + slots, slot).start()

        for q in range(1, n_inp):
            send_part(b, q).start()
        return carry

    lax.fori_loop(0, blocks, compute, 0)

    for copy in started:
        copy.wait_send()
    everything = [remote(parts.at[pl.ds(0, per_owner)], landed.at[q - 1], s_sems.at[q - 1],
                         r_sems.at[q - 1], (me_o, lax.rem(me_p + q, n_inp))) for q in range(1, n_inp)]
    for copy in everything:
        copy.wait_recv()
    for s in range(per_owner):
        total = parts[me_p * per_owner + s]
        for q in range(1, n_inp):
            total = total + landed[q - 1, s]
        out[s * cells_own:(s + 1) * cells_own, :] = total.T[0:cells_own, :].astype(out.dtype)
    for copy in everything:
        copy.wait_send()


def solution(mesh):
    n_out, n_inp = mesh.shape["out"], mesh.shape["inp"]
    nx = len({device.coords[0] for device in mesh.devices[:, 0]})

    def local(tensor, state):
        rows_out, rows_inp, width = tensor.shape
        cells_own = state.shape[0]
        cells = n_out * cells_own
        per_owner = n_out // n_inp
        padded = -(-cells_own // 128) * 128
        nz = n_out // nx
        return pl.pallas_call(
            functools.partial(kernel, nx, n_out, n_inp),
            out_shape=jax.ShapeDtypeStruct((cells // n_inp, rows_out), jnp.bfloat16),
            in_specs=[pl.BlockSpec(memory_space=pl.ANY), pl.BlockSpec(memory_space=pltpu.VMEM)],
            out_specs=pl.BlockSpec(memory_space=pltpu.VMEM),
            scratch_shapes=[
                pltpu.VMEM((n_out, cells_own, width), jnp.bfloat16),
                pltpu.VMEM((width, cells), jnp.bfloat16),
                pltpu.VMEM((rows_inp, cells), jnp.float32),
                pltpu.VMEM((SLOTS, GROUP, rows_inp, width), jnp.bfloat16),
                pltpu.VMEM((n_out, rows_out, padded), jnp.float32),
                pltpu.VMEM((n_inp - 1, per_owner, rows_out, padded), jnp.float32),
                pltpu.SemaphoreType.DMA((2,)),
                pltpu.SemaphoreType.DMA((2, nz)),
                pltpu.SemaphoreType.DMA((2, nx, nz)),
                pltpu.SemaphoreType.DMA((2, nx, nz)),
                pltpu.SemaphoreType.DMA((SLOTS,)),
                pltpu.SemaphoreType.DMA((n_inp - 1,)),
                pltpu.SemaphoreType.DMA((n_inp - 1,)),
            ],
            compiler_params=pltpu.CompilerParams(
                collective_id=0, has_side_effects=True, vmem_limit_bytes=60 * 2**20),
            name="collide",
        )(tensor, state)

    return jax.shard_map(
        local, mesh=mesh, in_specs=(P("out", "inp", None), P("out", None)),
        out_specs=P("inp", "out"), check_vma=False)
```

```python
import functools

import jax
import jax.numpy as jnp
from jax import lax
from jax.experimental import pallas as pl
from jax.experimental.pallas import tpu as pltpu
from jax.sharding import PartitionSpec as P

MESH = pl.DeviceIdType.MESH
GROUP = 16
SLOTS = 5


def flip(value, bits):
    for bit in (1 << n for n in range(bits.bit_length())):
        if bits & bit:
            value = value + bit * (1 - 2 * ((value // bit) % 2))
    return value


def kernel(nx, n_out, n_inp, tensor, state, out, gathered, turned, chosen, slab, parts, landed,
           z_sems, x_sems, core_sems, t_sems, s_sems, r_sems):
    rows_out, rows_inp, width = tensor.shape
    cells_own = state.shape[0]
    cells = n_out * cells_own
    nz = n_out // nx
    per_owner = n_out // n_inp
    group = slab.shape[1]
    blocks = rows_out // group
    slots = slab.shape[0]
    lanes = 256 if cells % 256 == 0 else cells
    halves = 2
    half_width = width // halves
    early = -(-lanes // cells_own)

    me_o = lax.axis_index("out")
    me_p = lax.axis_index("inp")
    z, x = me_o // nx, me_o % nx
    half = me_p % halves
    partner = me_p + 1 - 2 * half
    cols = pl.ds(pl.multiple_of(half * half_width, 128), half_width)

    def fetch(b, slot):
        return pltpu.make_async_copy(
            tensor.at[pl.ds(b * group, group)], slab.at[slot], t_sems.at[slot])

    for b in range(slots):
        fetch(b, b).start()

    def out_of(d, e):
        return flip(z, d) * nx + flip(x, e)

    barrier = pltpu.get_barrier_semaphore()
    near = [(out_of(d, 0), me_p) for d in range(1, nz)]
    near += [(out_of(0, e), me_p) for e in range(1, nx)]
    near += [(me_o, lax.rem(me_p + q, n_inp)) for q in range(1, n_inp)]
    for device in near:
        pl.semaphore_signal(barrier, inc=1, device_id=device, device_id_type=MESH)
    pl.semaphore_wait(barrier, len(near))

    def remote(src, dst, send, recv, device):
        return pltpu.make_async_remote_copy(
            src_ref=src, dst_ref=dst, send_sem=send, recv_sem=recv,
            device_id=device, device_id_type=MESH)

    def shard(d, e):
        return gathered.at[pl.ds((d * nx + e) * cells_own, cells_own), cols]

    def z_copy(d):
        return remote(state.at[:, cols], shard(d, 0), z_sems.at[0, d], z_sems.at[1, d],
                      (out_of(d, 0), me_p))

    def x_copy(e, d):
        return remote(state.at[:, cols] if d == 0 else shard(d, 0), shard(d, e),
                      x_sems.at[0, e, d], x_sems.at[1, e, d], (out_of(0, e), me_p))

    def core_copy(e, d):
        return remote(shard(d, e), shard(d, e), core_sems.at[0, e, d], core_sems.at[1, e, d],
                      (me_o, partner))

    def relay_x(d):
        for e in range(1, nx):
            x_copy(e, d).wait_recv()
            core_copy(e, d).start()

    def relay_z(d):
        z_copy(d).wait_recv()
        for e in range(1, nx):
            x_copy(e, d).start()
        core_copy(0, d).start()

    for e in range(1, nx):
        x_copy(e, 0).start()
    for d in range(1, nz):
        z_copy(d).start()
    gathered[0:cells_own, :] = state[...]
    relay_x(0)
    relay_z(1)
    order = [(d, e) for d in range(nz) for e in range(nx)]
    for d, e in order[1:early]:
        core_copy(e, d).wait_recv()

    first = pl.multiple_of(me_p * rows_inp, rows_inp)

    def turn(start, stop):
        for j in range(0, width, 128):
            turned[j:j + 128, start:stop] = gathered[start:stop, j:j + 128].T
        chosen[:, start:stop] = turned[pl.ds(first, rows_inp), start:stop].astype(jnp.float32)

    def send_part(b, q):
        owner = lax.rem(me_p + q, n_inp)
        rows = pl.ds(pl.multiple_of(b * group, group), group)
        return remote(parts.at[pl.ds(owner * per_owner, per_owner), rows],
                      landed.at[q - 1, :, rows],
                      s_sems.at[q - 1], r_sems.at[q - 1], (me_o, owner))

    def products(b, slot, start, stop):
        pieces = []
        for n in range(start, stop, lanes):
            sums = []
            for k in range(group):
                inner = jnp.dot(slab[slot, k], turned[:, n:n + lanes],
                                preferred_element_type=jnp.float32)
                sums.append(jnp.sum(inner * chosen[:, n:n + lanes], axis=0, keepdims=True))
            pieces.append(jnp.concatenate(sums, axis=0))
        total = jnp.concatenate(pieces, axis=1)
        rows = pl.ds(pl.multiple_of(b * group, group), group)
        for s, (d, e) in enumerate(order):
            low, high = max(start, s * cells_own), min(stop, (s + 1) * cells_own)
            if low < high:
                parts[out_of(d, e), rows, low - s * cells_own:high - s * cells_own] = (
                    total[:, low - start:high - start])

    def finish(b, slot):
        for q in range(1, n_inp):
            send_part(b, q).start()

        @pl.when(b + slots < blocks)
        def _():
            fetch(b + slots, slot).start()

    turn(0, lanes)

    def lead(b, carry):
        for d in range(2, nz + 1):
            @pl.when(b == min((d - 1) * slots // max(nz - 1, 1), slots - 1))
            def _():
                if d < nz:
                    relay_z(d)
                relay_x(d - 1)
        fetch(b, b).wait()
        products(b, b, 0, lanes)
        return carry

    lax.fori_loop(0, slots, lead, 0)
    for d, e in order[early:]:
        core_copy(e, d).wait_recv()
    if lanes < cells:
        turn(lanes, cells)

    def follow(b, carry):
        if lanes < cells:
            products(b, b, lanes, cells)
        finish(b, b)
        return carry

    lax.fori_loop(0, slots, follow, 0)

    def whole(b, carry):
        slot = lax.rem(b, slots)
        fetch(b, slot).wait()
        products(b, slot, 0, cells)
        finish(b, slot)
        return carry

    if slots < blocks:
        lax.fori_loop(slots, blocks, whole, 0)

    everything = [remote(parts.at[pl.ds(0, per_owner)], landed.at[q - 1], s_sems.at[q - 1],
                         r_sems.at[q - 1], (me_o, lax.rem(me_p + q, n_inp))) for q in range(1, n_inp)]
    for d in range(1, nz):
        z_copy(d).wait_send()
    for d, e in order:
        if e > 0:
            x_copy(e, d).wait_send()
        if (d, e) != (0, 0):
            core_copy(e, d).wait_send()
    for copy in everything:
        copy.wait_recv()
    for s in range(per_owner):
        total = parts[me_p * per_owner + s]
        for q in range(1, n_inp):
            total = total + landed[q - 1, s]
        out[s * cells_own:(s + 1) * cells_own, :] = total.T[0:cells_own, :].astype(out.dtype)
    for copy in everything:
        copy.wait_send()


def solution(mesh):
    n_out, n_inp = mesh.shape["out"], mesh.shape["inp"]
    nx = len({device.coords[0] for device in mesh.devices[:, 0]})

    def local(tensor, state):
        rows_out, rows_inp, width = tensor.shape
        cells_own = state.shape[0]
        cells = n_out * cells_own
        per_owner = n_out // n_inp
        padded = -(-cells_own // 128) * 128
        nz = n_out // nx
        group = min(GROUP, rows_out)
        slots = min(SLOTS, rows_out // group)
        return pl.pallas_call(
            functools.partial(kernel, nx, n_out, n_inp),
            out_shape=jax.ShapeDtypeStruct((cells // n_inp, rows_out), jnp.bfloat16),
            in_specs=[pl.BlockSpec(memory_space=pl.ANY), pl.BlockSpec(memory_space=pltpu.VMEM)],
            out_specs=pl.BlockSpec(memory_space=pltpu.VMEM),
            scratch_shapes=[
                pltpu.VMEM((cells, width), jnp.bfloat16),
                pltpu.VMEM((width, cells), jnp.bfloat16),
                pltpu.VMEM((rows_inp, cells), jnp.float32),
                pltpu.VMEM((slots, group, rows_inp, width), jnp.bfloat16),
                pltpu.VMEM((n_out, rows_out, padded), jnp.float32),
                pltpu.VMEM((n_inp - 1, per_owner, rows_out, padded), jnp.float32),
                pltpu.SemaphoreType.DMA((2, nz)),
                pltpu.SemaphoreType.DMA((2, nx, nz)),
                pltpu.SemaphoreType.DMA((2, nx, nz)),
                pltpu.SemaphoreType.DMA((slots,)),
                pltpu.SemaphoreType.DMA((n_inp - 1,)),
                pltpu.SemaphoreType.DMA((n_inp - 1,)),
            ],
            compiler_params=pltpu.CompilerParams(
                collective_id=0, has_side_effects=True, vmem_limit_bytes=60 * 2**20),
            name="collide",
        )(tensor, state)

    return jax.shard_map(
        local, mesh=mesh, in_specs=(P("out", "inp", None), P("out", None)),
        out_specs=P("inp", "out"), check_vma=False)
```
